512 devices in a mesh: rep: 4 (over y_hi, core), shard: 128 (over y_lo, z, x).
Axes of the slice: x: 4, y: 4 (y_hi: 2, y_lo: 2; y = y_hi * 2 + y_lo), z: 16, core: 2. Of those that a mesh axis runs over, the one named last changes fastest.
Arguments:
- gradients: float32 [4, 128, 8, 5120], P('rep', 'shard'), may hold values from -6 to 6
- master: float32 [128, 8, 5120], P('shard', 'rep'), may hold values from -6 to 6
- first_moment: float32 [128, 8, 5120], P('shard', 'rep'), may hold values from -4 to 4
- second_moment: float32 [128, 8, 5120], P('shard', 'rep'), may hold values from 0.001 to 0.01
- old_ratio: float32 [128], replicated, may hold values from 0.5 to 2
- group_owner: int32 [128], replicated, may hold values from 0 to 127, each once
- layer_group: int32 [128], replicated, may hold values from 0 to 127, each once
Outputs:
- new_master: float32 [128, 8, 5120], P('shard', 'rep')
- new_first: float32 [128, 8, 5120], P('shard', 'rep')
- new_second: float32 [128, 8, 5120], P('shard', 'rep')
- replica: bfloat16 [128, 8, 5120], P(None, 'rep')
- new_ratio: float32 [128], replicated
The draws below stay inside these ranges and needn't reach their ends.
Inputs may be any that keep to these rules, and one draw needn't show every extreme that they name: `group_owner`: every device owns exactly one group. `layer_group`: every group holds exactly one layer.
All inputs are finite; a program needn't handle non-finite values.
Results may differ from the reference program's by a relative error of at most 0.0004.
Values may be sent and summed in bfloat16 or wider, within the bound.
A program may use at most 64 MiB of HBM per device.

```python
import math
import jax
import jax.numpy as jnp
from jax import lax

FF = 5120
ROWS = 8
LAYERS = 128
N_REP = 4
N_SHARD = 128


def level_of(own_key, extent, split, low, top_value):
    factor_of = 1.0
    for dim, parts in split:
        steps = jax.random.uniform(jax.random.fold_in(jax.random.fold_in(own_key, 6), dim), (parts,), jnp.float32, low / len(split), top_value / len(split))
        factor_of = factor_of * jnp.repeat(jnp.exp(steps), extent[dim] // parts).reshape((-1,) + (1,) * (len(extent) - 1 - dim))
    return factor_of


def scatter_about(key, dims, deviation, limit, pieces=(), dtype=jnp.bfloat16):
    entries = deviation * jax.random.normal(key, dims, jnp.float32)
    if pieces:
        entries = entries * level_of(key, dims, pieces, -0.22, 0.18)
    return jnp.clip(entries, -limit, limit).astype(dtype)


def setup_inputs(seed: int = 0) -> dict:
    keys = jax.random.split(jax.random.key(seed), 8)
    return {
        "gradients": scatter_about(keys[0], (N_REP, N_SHARD, ROWS, FF), 1.0, 6.0, ((0, 4), (1, 128)), jnp.float32),
        "master": scatter_about(keys[1], (N_SHARD, ROWS, FF), 1.0, 6.0, ((0, 128), (1, 4)), jnp.float32),
        "first_moment": scatter_about(keys[2], (N_SHARD, ROWS, FF), 0.3, 4.0, ((0, 128), (1, 4)), jnp.float32),
        "second_moment": jnp.clip(jnp.exp(math.log(0.01) - 2.30258502 * jax.random.uniform(keys[3], (N_SHARD, ROWS, FF), jnp.float32) ** level_of(keys[3], (N_SHARD, ROWS, FF), ((0, 128), (1, 4)), -0.2, 0.2)), 0.001, 0.01),
        "old_ratio": jnp.clip(jnp.exp(jax.random.uniform(keys[4], (LAYERS,), jnp.float32, math.log(0.5), math.log(2.0))), 0.5, 2.0),
        "group_owner": jax.random.permutation(keys[5], N_SHARD).astype(jnp.int32),
        "layer_group": jax.random.permutation(keys[6], LAYERS).astype(jnp.int32),
    }


def reference(gradients, master, first_moment, second_moment, old_ratio, group_owner, layer_group):
    holder = group_owner[layer_group].astype(jnp.int32)
    summed = lax.optimization_barrier(jnp.sum(gradients, axis=0))
    slot_ratio = jnp.zeros((master.shape[0],), jnp.float32).at[holder].set(old_ratio)
    new_first = 0.9 * first_moment + 0.1 * summed
    new_second = 0.999 * second_moment + 0.001 * summed * summed
    update = new_first / (1.0 - 0.9 ** 10) / (jnp.sqrt(new_second / (1.0 - 0.999 ** 10)) + 1e-06) + 0.1 * master
    new_master = master - 0.1 * slot_ratio[:, None, None] * update
    weight_sq = lax.optimization_barrier(jnp.sum(master * master, axis=(1, 2)))
    update_sq = lax.optimization_barrier(jnp.sum(update * update, axis=(1, 2)))
    new_ratio = jnp.sqrt(weight_sq[holder]) / (jnp.sqrt(update_sq[holder]) + 1e-06)
    replica = new_master.astype(jnp.bfloat16)[holder]
    return (new_master, new_first, new_second, replica, new_ratio)
```

```python
import functools

import jax
import jax.numpy as jnp
from jax import lax
from jax.experimental import pallas as pl
from jax.experimental.pallas import tpu as pltpu
from jax.sharding import Mesh
from jax.sharding import PartitionSpec as P

REP = ("rep_0", "rep_1")
SHARD = ("shard_0", "shard_1", "shard_2")
NX, NY, NZ = 4, 2, 16
SLOTS = NX * NY * NZ
MESH = pl.DeviceIdType.MESH

SCHEDULE = (
    ((0, 0, 0), ((0, 0, -1), (0, 0, 2), (0, 0, 5), (0, 0, -5), (0, 0, 8), (-1, 0, 0), (0, 0, 1), (2, 0, 0), (1, 0, 0), (0, 1, 0),)),
    ((0, 0, -1), ((0, 0, -4), (0, 1, -1), (2, 0, -1), (0, 0, -2), (1, 0, -1), (-1, 0, -1),)),
    ((-1, 0, 0), ((-1, 0, 1), (-1, 1, 0),)),
    ((0, 1, 0), ()),
    ((1, 0, 0), ((1, 1, 0),)),
    ((0, 0, 2), ((0, 1, 2), (2, 0, 2), (0, 0, 3), (-1, 0, 2), (1, 0, 2),)),
    ((2, 0, 0), ((2, 1, 0), (2, 0, 1),)),
    ((0, 0, -5), ((0, 1, -5), (0, 0, -7), (1, 0, -5), (-1, 0, -5), (0, 0, -6),)),
    ((0, 1, -1), ((0, 1, -2), (-1, 1, -1), (1, 1, -1),)),
    ((-1, 0, -1), ()),
    ((1, 0, -1), ((1, 0, -2),)),
    ((-1, 1, 0), ()),
    ((0, 0, 5), ((0, 0, 7), (2, 0, 5), (0, 1, 5), (-1, 0, 5), (0, 0, 6), (1, 0, 5),)),
    ((2, 0, -1), ((2, 1, -1), (2, 0, -2),)),
    ((1, 1, 0), ()),
    ((-1, 0, 2), ((-1, 0, 3),)),
    ((1, 0, 2), ()),
    ((0, 0, 1), ((1, 0, 1), (0, 1, 1),)),
    ((0, 1, 2), ((-1, 1, 2), (1, 1, 2),)),
    ((2, 0, 2), ((2, 0, 3),)),
    ((2, 1, 0), ((2, 1, 1),)),
    ((-1, 0, 1), ((-1, 1, 1),)),
    ((0, 0, -4), ((-1, 0, -4), (1, 0, -4),)),
    ((0, 0, 8), ((0, 1, 8), (-1, 0, 8), (1, 0, 8),)),
    ((0, 0, -2), ((-1, 0, -2), (0, 0, -3),)),
    ((0, 0, 3), ((1, 0, 3), (0, 1, 3), (0, 0, 4),)),
    ((2, 0, 1), ()),
    ((-1, 0, -5), ((-1, 1, -5), (2, 0, -5),)),
    ((1, 0, -5), ((1, 0, -6), (1, 1, -5),)),
    ((0, 1, -5), ((2, 1, -5), (0, 1, -6),)),
    ((-1, 1, -1), ((-1, 1, -2),)),
    ((1, 1, -1), ((1, 1, -2),)),
    ((0, 1, 5), ((-1, 1, 5), (1, 1, 5), (0, 1, 6),)),
    ((0, 0, -7), ((0, 1, -7), (-1, 0, -7), (1, 0, -7),)),
    ((-1, 0, 5), ((-1, 0, 6),)),
    ((1, 0, 5), ()),
    ((2, 1, -1), ((2, 1, -2),)),
    ((0, 0, -6), ((-1, 0, -6),)),
    ((0, 0, 7), ((0, 1, 7), (-1, 0, 7), (1, 0, 7),)),
    ((0, 1, 1), ()),
    ((0, 1, -2), ((0, 1, -3),)),
    ((2, 0, 5), ((2, 0, 6), (2, 1, 5),)),
    ((1, 0, 1), ((1, 1, 1),)),
    ((-1, 1, 2), ((-1, 1, 3), (2, 1, 2),)),
    ((0, 0, 6), ((1, 0, 6),)),
    ((1, 0, -2), ((1, 0, -3),)),
    ((-1, 1, 1), ()),
    ((1, 1, 2), ((1, 1, 3),)),
    ((-1, 0, -4), ((-1, 1, -4), (2, 0, -4),)),
    ((-1, 0, 3), ()),
    ((2, 0, -2), ((2, 0, -3),)),
    ((0, 1, 8), ((1, 1, 8),)),
    ((1, 0, -4), ((1, 1, -4),)),
    ((-1, 0, 8), ((-1, 1, 8),)),
    ((2, 0, 3), ((2, 0, 4), (2, 1, 3),)),
    ((0, 0, -3), ()),
    ((0, 1, 3), ((0, 1, 4),)),
    ((-1, 0, -2), ((-1, 0, -3),)),
    ((1, 0, 8), ((2, 0, 8),)),
    ((2, 1, 1), ()),
    ((1, 0, -6), ((2, 0, -6), (1, 1, -6),)),
    ((-1, 1, -5), ((-1, 1, -6),)),
    ((1, 0, 3), ((1, 0, 4),)),
    ((2, 0, -5), ()),
    ((0, 0, 4), ((-1, 0, 4),)),
    ((0, 1, -6), ()),
    ((1, 1, -5), ()),
    ((0, 1, 6), ()),
    ((-1, 1, 5), ((-1, 1, 6),)),
    ((1, 1, 5), ((1, 1, 6),)),
    ((-1, 1, -2), ((-1, 1, -3),)),
    ((0, 1, -7), ((2, 1, -7),)),
    ((-1, 0, 6), ()),
    ((1, 1, -2), ((1, 1, -3),)),
    ((2, 1, -5), ((2, 1, -6),)),
    ((0, 1, 7), ((-1, 1, 7), (1, 1, 7), (2, 1, 7),)),
    ((-1, 0, -7), ((2, 0, -7), (-1, 1, -7),)),
    ((1, 0, -7), ((1, 1, -7),)),
    ((2, 0, 6), ((2, 1, 6), (2, 0, 7),)),
    ((2, 1, -2), ((2, 1, -3),)),
    ((2, 1, 5), ()),
    ((-1, 0, -6), ()),
    ((1, 0, 7), ()),
    ((-1, 1, 3), ((-1, 1, 4),)),
    ((0, 1, -3), ((0, 1, -4),)),
    ((1, 1, 1), ()),
    ((1, 0, 6), ()),
    ((-1, 0, 7), ()),
    ((1, 1, 3), ((1, 1, 4),)),
    ((1, 0, -3), ()),
    ((-1, 1, -4), ((2, 1, -4),)),
    ((2, 1, 2), ()),
    ((1, 1, 8), ((2, 1, 8),)),
    ((2, 0, 4), ((2, 1, 4),)),
    ((2, 0, -3), ()),
    ((1, 1, -4), ()),
    ((2, 0, -4), ()),
    ((2, 0, 8), ()),
    ((0, 1, 4), ()),
    ((-1, 0, -3), ()),
    ((-1, 1, 8), ()),
    ((-1, 0, 4), ()),
    ((2, 0, -6), ()),
    ((1, 0, 4), ()),
    ((-1, 1, -6), ()),
    ((2, 1, 3), ()),
    ((-1, 1, 6), ()),
    ((-1, 1, -3), ()),
    ((1, 1, -6), ()),
    ((1, 1, 6), ()),
    ((1, 1, -3), ()),
    ((-1, 1, -7), ()),
    ((2, 1, -7), ()),
    ((2, 0, 7), ()),
    ((2, 1, -6), ()),
    ((-1, 1, 7), ()),
    ((1, 1, 7), ()),
    ((1, 1, -7), ()),
    ((-1, 1, 4), ()),
    ((2, 1, -3), ()),
    ((2, 1, 7), ()),
    ((2, 1, 6), ()),
    ((2, 0, -7), ()),
    ((1, 1, 4), ()),
    ((0, 1, -4), ()),
    ((2, 1, 8), ()),
    ((2, 1, 4), ()),
    ((2, 1, -4), ()),
)

PLACES = {row[0]: k for k, row in enumerate(SCHEDULE)}


def step_kernel(
    grad, master, first, second, ratio, owner, group, owner_s, group_s,
    new_master, new_first, new_second, replica, new_ratio,
    gv, parts, mv, fv, sv, rv, ov, lv, os_, ls_, own, buf, stats, table,
    in_sem, rs_send, rs_recv, st_send, st_recv, z_send, z_recv, p_send, p_recv, ag_send, ag_recv,
):
    yh, core, yl, z, x = (lax.axis_index(a) for a in (*REP, *SHARD))
    rep = yh * 2 + core

    def at(dx, dy, dz):
        return (yh, core, lax.rem(yl + dy + 2, NY), lax.rem(z + dz + NZ, NZ), lax.rem(x + dx + NX, NX))

    def slot(dx, dy, dz):
        return lax.rem(yl - dy + 2, NY) * (NZ * NX) + lax.rem(z - dz + NZ, NZ) * NX + lax.rem(x - dx + NX, NX)

    peers = (
        (yh, 1 - core, yl, z, x),
        (1 - yh, core, yl, z, x),
        (1 - yh, 1 - core, yl, z, x),
    )
    line = [(0, 0, dz) for dz in range(1, NZ)]
    plane = [(dx, dy, 0) for dy in range(NY) for dx in range(NX) if dx or dy]

    barrier = pltpu.get_barrier_semaphore()
    partners = [*peers, *(at(*d) for d in line), *(at(*d) for d in plane)]
    for p in partners:
        pl.semaphore_signal(barrier, inc=1, device_id=p, device_id_type=MESH)
    loads = [
        pltpu.make_async_copy(src, dst, in_sem.at[k])
        for k, (src, dst) in enumerate((
            (grad.at[0, 0], gv), (master.at[0], mv), (first.at[0], fv), (second.at[0], sv),
            (ratio, rv), (owner, ov), (group, lv), (owner_s, os_), (group_s, ls_),
        ))
    ]
    for c in loads:
        c.start()
    loads[0].wait()
    for r in range(4):
        parts[r] = gv[2 * r : 2 * r + 2, :]
    pl.semaphore_wait(barrier, len(partners))

    rs = []
    for k, p in enumerate(peers):
        c = pltpu.make_async_remote_copy(
            src_ref=parts.at[p[0] * 2 + p[1]], dst_ref=gv_in(parts, k), send_sem=rs_send.at[k], recv_sem=rs_recv.at[k],
            device_id=p, device_id_type=MESH,
        )
        c.start()
        rs.append(c)
    for c in loads[1:]:
        c.wait()

    me = yl * (NZ * NX) + z * NX + x
    lane = lax.broadcasted_iota(jnp.int32, (1, SLOTS), 1)
    my_group = jnp.sum(jnp.where(ov[...] == me, lane, 0), axis=1, keepdims=True)
    my_ratio = jnp.sum(jnp.where(lv[...] == my_group, rv[...], 0.0), axis=1, keepdims=True)

    for c in rs:
        c.wait_recv()
    ff = mv.shape[1]
    width = ff // 8
    w_acc = jnp.zeros((2, width), jnp.float32)
    u_acc = jnp.zeros((2, width), jnp.float32)
    for b in range(8):
        cols = slice(b * width, (b + 1) * width)
        summed = parts[rep, :, cols] + parts[4, :, cols] + parts[5, :, cols] + parts[6, :, cols]
        w = mv[:, cols]
        nf = 0.9 * fv[:, cols] + 0.1 * summed
        ns = 0.999 * sv[:, cols] + 0.001 * summed * summed
        up = nf / (1.0 - 0.9**10) / (jnp.sqrt(ns / (1.0 - 0.999**10)) + 1e-06) + 0.1 * w
        nw = w - 0.1 * my_ratio * up
        buf[me, :, cols] = nw.astype(jnp.bfloat16)
        new_master[0, :, cols] = nw
        new_first[0, :, cols] = nf
        new_second[0, :, cols] = ns
        w_acc += w * w
        u_acc += up * up

    def send_on(o, children):
        block = buf.at[slot(*o)]
        for c in children:
            d = tuple(b - a for a, b in zip(o, c))
            pltpu.make_async_remote_copy(
                src_ref=block, dst_ref=block, send_sem=ag_send, recv_sem=ag_recv.at[PLACES[c]],
                device_id=at(*d), device_id_type=MESH,
            ).start()

    send_on(*SCHEDULE[0])

    row = lax.broadcasted_iota(jnp.int32, (2, SLOTS), 0)
    w_sum = jnp.sum(w_acc, axis=(0, 1), keepdims=True)
    u_sum = jnp.sum(u_acc, axis=(0, 1), keepdims=True)
    stats[3] = jnp.where(row == 0, w_sum, u_sum)
    st = []
    for k, p in enumerate(peers):
        c = pltpu.make_async_remote_copy(
            src_ref=stats.at[3], dst_ref=stats.at[k], send_sem=st_send.at[k], recv_sem=st_recv.at[k],
            device_id=p, device_id_type=MESH,
        )
        c.start()
        st.append(c)

    here = yl * NX + x

    def stats_to_line():
        for c in st:
            c.wait_recv()
        table[here, z] = stats[0] + stats[1] + stats[2] + stats[3]
        for d in line:
            pltpu.make_async_remote_copy(
                src_ref=table.at[here, z], dst_ref=table.at[here, z], send_sem=z_send, recv_sem=z_recv,
                device_id=at(*d), device_id_type=MESH,
            ).start()

    def stats_to_plane():
        some = table.at[0, 0 : NZ - 1]
        pltpu.make_async_copy(some, some, z_recv).wait()
        for d in plane:
            pltpu.make_async_remote_copy(
                src_ref=table.at[here], dst_ref=table.at[here], send_sem=p_send, recv_sem=p_recv,
                device_id=at(*d), device_id_type=MESH,
            ).start()

    def wait_for(o):
        block = buf.at[slot(*o)]
        pltpu.make_async_copy(block, block, ag_recv.at[PLACES[o]]).wait()

    for k, (o, children) in enumerate(SCHEDULE[1:]):
        if k == LINE_AT:
            stats_to_line()
        if k == PLANE_AT:
            stats_to_plane()
        wait_for(o)
        send_on(o, children)

    some = table.at[0 : NX * NY - 1]
    pltpu.make_async_copy(some, some, p_recv).wait()

    sub = lax.broadcasted_iota(jnp.int32, (SLOTS, SLOTS), 0)
    lan = lax.broadcasted_iota(jnp.int32, (SLOTS, SLOTS), 1)
    owner_col = jnp.sum(jnp.where(sub == lan, ov[...], 0), axis=1, keepdims=True)
    holder = jnp.sum(jnp.where(sub == lv[...], owner_col, 0), axis=0, keepdims=True)
    place = ((holder // (NZ * NX)) * NX + lax.rem(holder, NX)) * NZ + lax.rem(holder // NX, NZ)
    picked = jnp.zeros((2, SLOTS), jnp.float32)
    for p in range(SLOTS):
        picked = jnp.where(place == p, table[p // NZ, p % NZ], picked)
    new_ratio[...] = jnp.sqrt(picked[0:1]) / (jnp.sqrt(picked[1:2]) + 1e-06)

    def put(l, carry):
        replica[l] = buf[os_[ls_[l]]]
        return carry

    lax.fori_loop(0, SLOTS, put, 0, unroll=8)

    for c in rs:
        c.wait_send()
    for c in st:
        c.wait_send()
    some = table.at[0, 0 : NZ - 1]
    pltpu.make_async_copy(some, some, z_send).wait()
    some = table.at[0 : NX * NY - 1]
    pltpu.make_async_copy(some, some, p_send).wait()
    some = buf.at[0 : SLOTS - 1]
    pltpu.make_async_copy(some, some, ag_send).wait()


def gv_in(parts, k):
    return parts.at[4 + k]


LINE_AT = 8
PLANE_AT = 60


def flush_kernel(a, b, c, d, e, a_out, b_out, c_out, d_out, e_out, sem):
    copies = [
        pltpu.make_async_copy(src, dst, sem.at[k])
        for k, (src, dst) in enumerate(((d, d_out), (a, a_out), (b, b_out), (c, c_out), (e, e_out)))
    ]
    for copy in copies:
        copy.start()
    for copy in copies:
        copy.wait()


def on_device(gradients, master, first_moment, second_moment, old_ratio, group_owner, layer_group):
    ff = master.shape[2]
    f32, i32 = jnp.float32, jnp.int32
    hbm, vmem = pl.BlockSpec(memory_space=pltpu.HBM), pl.BlockSpec(memory_space=pltpu.VMEM)
    shapes = (
        jax.ShapeDtypeStruct(master.shape, f32),
        jax.ShapeDtypeStruct(master.shape, f32),
        jax.ShapeDtypeStruct(master.shape, f32),
        jax.ShapeDtypeStruct((SLOTS, 2, ff), jnp.bfloat16),
        jax.ShapeDtypeStruct((1, SLOTS), f32),
    )
    dma = pltpu.SemaphoreType.DMA
    results = pl.pallas_call(
        step_kernel,
        out_shape=shapes,
        in_specs=[hbm] * 9,
        out_specs=[vmem] * 5,
        scratch_shapes=[
            pltpu.VMEM((8, ff), f32),
            pltpu.VMEM((7, 2, ff), f32),
            pltpu.VMEM((2, ff), f32),
            pltpu.VMEM((2, ff), f32),
            pltpu.VMEM((2, ff), f32),
            pltpu.VMEM((1, SLOTS), f32),
            pltpu.VMEM((1, SLOTS), i32),
            pltpu.VMEM((1, SLOTS), i32),
            pltpu.SMEM((SLOTS,), i32),
            pltpu.SMEM((SLOTS,), i32),
            pltpu.VMEM((2, ff), jnp.bfloat16),
            pltpu.VMEM((SLOTS, 2, ff), jnp.bfloat16),
            pltpu.VMEM((4, 2, SLOTS), f32),
            pltpu.VMEM((NX * NY, NZ, 2, SLOTS), f32),
            dma((9,)),
            dma((3,)),
            dma((3,)),
            dma((3,)),
            dma((3,)),
            dma,
            dma,
            dma,
            dma,
            dma,
            dma((SLOTS,)),
        ],
        compiler_params=pltpu.CompilerParams(
            collective_id=0, has_side_effects=True, vmem_limit_bytes=24 << 20
        ),
        name="lamb_step",
    )(
        gradients, master, first_moment, second_moment,
        old_ratio.reshape(1, SLOTS), group_owner.reshape(1, SLOTS), layer_group.reshape(1, SLOTS),
        group_owner, layer_group,
    )
    a, b, c, d, e = pl.pallas_call(
        flush_kernel,
        out_shape=shapes,
        in_specs=[vmem] * 5,
        out_specs=[hbm] * 5,
        scratch_shapes=[dma((5,))],
        compiler_params=pltpu.CompilerParams(vmem_limit_bytes=16 << 20),
        name="lamb_flush",
    )(*results)
    return a, b, c, d, e.reshape(SLOTS)


def solution(mesh):
    torus = Mesh(mesh.devices.reshape(2, 2, NY, NZ, NX), (*REP, *SHARD))
    placed = (
        P(REP, SHARD, None, None),
        P(SHARD, REP, None),
        P(SHARD, REP, None),
        P(SHARD, REP, None),
        P(),
        P(),
        P(),
    )
    return jax.shard_map(
        on_device,
        mesh=torus,
        in_specs=placed,
        out_specs=(P(SHARD, REP, None), P(SHARD, REP, None), P(SHARD, REP, None), P(None, REP, None), P()),
        check_vma=False,
    )
```
